16 devices in a mesh: side: 2 (over z), rep: 8 (over y, x, core).
Axes of the slice: x: 2, y: 2, z: 2, core: 2. Of those that a mesh axis runs over, the one named last changes fastest.
Arguments:
- w_up: float32 [2, 6, 896, 4864], P('side', None, 'rep')
- w_down: float32 [2, 6, 4864, 896], P('side', None, None, 'rep')
- g_up: float32 [2, 6, 896, 4864], P('side', None, 'rep')
- g_down: float32 [2, 6, 4864, 896], P('side', None, None, 'rep')
- learn_rate: float32 [], replicated
- prompts: bfloat16 [2, 32768, 896], P('side', 'rep')
- prompt_lens: int32 [8], P('rep')
Outputs:
- output 1: float32 [2, 6, 896, 4864], P('side', None, 'rep')
- output 2: float32 [2, 6, 4864, 896], P('side', None, None, 'rep')
- output 3: bfloat16 [2, 32768, 896], P('side', 'rep')
All inputs are finite; a program needn't handle non-finite values.
Results may differ from the reference program's by a relative error of at most 0.0103396.
Values are sent between devices in bfloat16 or wider.
A program may use at most 1 GiB of HBM per device.

```python
import jax
import jax.numpy as jnp
from jax import lax

SIDE_DEVS = 2
REP_DEVS = 8
MODEL_DIM = 896
FFN_DIM = 4864
LAYERS = 6
TOKENS = 4096
TP_WAYS = SIDE_DEVS // 2
FF_PIECE = FFN_DIM // TP_WAYS
D_PIECE = MODEL_DIM // TP_WAYS


def draw_lens(len_key):
    key_a, key_b = jax.random.split(len_key)
    low_len = max(1, TOKENS // 32)
    base_lens = jax.random.randint(key_a, (REP_DEVS,), low_len, TOKENS + 1, jnp.int32)
    full_slot = jax.random.randint(key_b, (), 0, REP_DEVS, jnp.int32)
    return jnp.where(jnp.arange(REP_DEVS) == full_slot, TOKENS, base_lens).astype(jnp.int32)


def setup_inputs(seed: int = 0) -> dict:
    sub_keys = jax.random.split(jax.random.key(seed), 7)
    up_shape = (TP_WAYS, LAYERS, MODEL_DIM, FF_PIECE)
    down_shape = (TP_WAYS, LAYERS, FF_PIECE, MODEL_DIM)
    up_scale = MODEL_DIM ** -0.5
    down_scale = 0.7 * FFN_DIM ** -0.5
    w_up = jax.random.normal(sub_keys[0], up_shape, jnp.float32) * up_scale
    w_down = jax.random.normal(sub_keys[1], down_shape, jnp.float32) * down_scale
    g_up = jax.random.normal(sub_keys[2], up_shape, jnp.float32) * up_scale
    g_down = jax.random.normal(sub_keys[3], down_shape, jnp.float32) * down_scale
    learn_rate = jax.random.uniform(sub_keys[4], (), jnp.float32, 0.02, 0.25)
    gen_rows = jax.random.normal(sub_keys[5], (TP_WAYS, REP_DEVS * TOKENS, D_PIECE), jnp.float32)
    prompts = jnp.concatenate([jnp.zeros_like(gen_rows), gen_rows], axis=0).astype(jnp.bfloat16)
    return {
        "w_up": jnp.concatenate([w_up, jnp.zeros_like(w_up)], axis=0),
        "w_down": jnp.concatenate([w_down, jnp.zeros_like(w_down)], axis=0),
        "g_up": jnp.concatenate([g_up, jnp.zeros_like(g_up)], axis=0),
        "g_down": jnp.concatenate([g_down, jnp.zeros_like(g_down)], axis=0),
        "learn_rate": learn_rate,
        "prompts": prompts,
        "prompt_lens": draw_lens(sub_keys[6]),
    }


def reference(w_up, w_down, g_up, g_down, learn_rate, prompts, prompt_lens):
    new_up = w_up - learn_rate * g_up
    new_down = w_down - learn_rate * g_down
    up_bf = new_up[:TP_WAYS].astype(jnp.bfloat16)
    down_bf = new_down[:TP_WAYS].astype(jnp.bfloat16)
    up_full = jnp.transpose(up_bf, (1, 2, 0, 3)).reshape(LAYERS, MODEL_DIM, FFN_DIM)
    down_full = jnp.transpose(down_bf, (1, 0, 2, 3)).reshape(LAYERS, FFN_DIM, MODEL_DIM)
    x_full = jnp.transpose(prompts[TP_WAYS:], (1, 0, 2)).reshape(REP_DEVS, TOKENS, MODEL_DIM)

    def layer_step(h_rows, layer_w):
        up_layer, down_layer = layer_w
        pre_act = jnp.dot(h_rows, up_layer, preferred_element_type=jnp.float32)
        act_bf = jax.nn.gelu(pre_act, approximate=True).astype(jnp.bfloat16)
        part_sum = jnp.dot(act_bf, down_layer, preferred_element_type=jnp.float32)
        return (h_rows.astype(jnp.float32) + part_sum).astype(jnp.bfloat16), None

    def one_replica(replica_in):
        row_block, length = replica_in
        h_rows, _ = lax.scan(layer_step, row_block, (up_full, down_full))
        keep_mask = jnp.arange(TOKENS)[:, None] < length
        return jnp.where(keep_mask, h_rows, jnp.zeros_like(h_rows))

    y_full = lax.map(one_replica, (x_full, prompt_lens))
    y_gen = jnp.transpose(y_full.reshape(REP_DEVS * TOKENS, TP_WAYS, D_PIECE), (1, 0, 2))
    outputs = jnp.concatenate([jnp.zeros_like(y_gen), y_gen], axis=0)
    return new_up, new_down, outputs
```

```python
import functools

import jax
import jax.numpy as jnp
from jax import lax
from jax.experimental import pallas as pl
from jax.experimental.pallas import tpu as pltpu
from jax.sharding import PartitionSpec as P

ROOT_2_PI = 0.7978845608
CUBIC = 0.044715 * ROOT_2_PI


def gelu(z):
    half = 0.5 * z
    return half + half * jnp.tanh(z * (ROOT_2_PI + CUBIC * (z * z)))


def cuts(total, step):
    return [(at, min(step, total - at)) for at in range(0, total, step)]


def layer_kernel(h_ref, up_ref, down_ref, out_ref, act_ref):
    width = h_ref.shape[1]
    for at, size in cuts(up_ref.shape[1], 512):
        z = jnp.dot(h_ref[...], up_ref[:, at : at + size], preferred_element_type=jnp.float32)
        act_ref[:, at : at + size] = gelu(z).astype(jnp.bfloat16)
    for at, size in cuts(width, 256):
        p = lax.dot_general(
            act_ref[...], down_ref[at : at + size, :], (((1,), (1,)), ((), ())), preferred_element_type=jnp.float32
        )
        out_ref[:, at : at + size] = (h_ref[:, at : at + size].astype(jnp.float32) + p).astype(jnp.bfloat16)


def mlp_layer(h, weights):
    rows, width = h.shape
    ffn = weights.shape[2]
    block = 512

    def matrix(which):
        return pl.BlockSpec((pl.Squeezed(), width, ffn), lambda i: (which, 0, 0), pipeline_mode=pl.Buffered(1))

    return pl.pallas_call(
        layer_kernel,
        grid=(rows // block,),
        in_specs=[pl.BlockSpec((block, width), lambda i: (i, 0)), matrix(0), matrix(1)],
        out_specs=pl.BlockSpec((block, width), lambda i: (i, 0)),
        out_shape=jax.ShapeDtypeStruct((rows, width), jnp.bfloat16),
        scratch_shapes=[pltpu.VMEM((block, ffn), jnp.bfloat16)],
        compiler_params=pltpu.CompilerParams(vmem_limit_bytes=48 * 2**20),
        cost_estimate=pl.CostEstimate(
            flops=4 * rows * width * ffn, bytes_accessed=4 * (rows + ffn) * width, transcendentals=rows * ffn
        ),
        name="mlp_layer",
    )(h, weights, weights)


def solution(mesh):
    up_spec = P("side", None, "rep", None)
    down_spec = P("side", None, None, "rep")
    act_spec = P("side", "rep", None)

    def device_step(w_up, w_down, g_up, g_down, learn_rate, prompts, prompt_lens):
        is_gen = lax.axis_index("side") == 1
        layers = w_up.shape[1]
        tokens = prompts.shape[1]
        half = tokens // 2
        new_up = w_up - learn_rate * g_up
        new_down = w_down - learn_rate * g_down
        up_bf = new_up[0].astype(jnp.bfloat16)
        down_bf = jnp.swapaxes(new_down[0], 1, 2).astype(jnp.bfloat16)
        own = [jnp.stack([up_bf[layer], down_bf[layer]]) for layer in range(layers)]
        moved = lax.ppermute(prompts[0, half:], "side", [(1, 0)])
        hidden = jnp.where(is_gen, prompts[0, :half], moved)

        def cross(own):
            return jnp.where(is_gen, lax.ppermute(own, "side", [(0, 1)]), own)

        def gather(staged):
            return lax.all_gather(staged, "rep", axis=1, tiled=True)

        staged = [cross(own[0]), cross(own[1]), cross(own[2])]
        gathered = [gather(staged[0]), gather(staged[1])]
        for layer in range(layers):
            hidden = mlp_layer(hidden, gathered[layer])
            if layer + 2 < layers:
                later = own[min(layer + 3, layers - 1)]
                hidden, ready, later = lax.optimization_barrier((hidden, staged[layer + 2], later))
                gathered.append(gather(ready))
                if layer + 3 < layers:
                    staged.append(cross(later))
        back = lax.ppermute(hidden, "side", [(0, 1)])
        out = jnp.concatenate([hidden, back], axis=0)
        keep = (jnp.arange(tokens)[:, None] < prompt_lens[0]) & is_gen
        out = jnp.where(keep, out, jnp.zeros_like(out))
        return new_up, new_down, out[None]

    return jax.shard_map(
        device_step,
        mesh=mesh,
        in_specs=(up_spec, down_spec, up_spec, down_spec, P(), act_spec, P("rep")),
        out_specs=(up_spec, down_spec, act_spec),
        check_vma=False,
    )
```

```python
import functools

import jax
import jax.numpy as jnp
from jax import lax
from jax.experimental import pallas as pl
from jax.experimental.pallas import tpu as pltpu
from jax.sharding import PartitionSpec as P

ROOT_2_PI = 0.7978845608
CUBIC = 0.044715 * ROOT_2_PI
MESH = pl.DeviceIdType.MESH
BLOCK = 512
GEN_BLOCKS = 5
Z, X, Y, DIAG, SIB, SIB_X, SIB_Y, SIB_DIAG = range(8)
SLOTS = 8


def gelu(z):
    half = 0.5 * z
    return half + half * jnp.tanh(z * (ROOT_2_PI + CUBIC * (z * z)))


def cuts(total, step):
    return [(at, min(step, total - at)) for at in range(0, total, step)]


def stack_kernel(
    up_ref, down_ref, x_ref, full_ref, y_ref, w_buf, act, h, send, recv, load, x_sem, y_send, y_recv, y_local
):
    layers, piece, ffn = up_ref.shape
    width = x_ref.shape[1]
    tokens = x_ref.shape[0]
    blocks = tokens // BLOCK
    far_blocks = blocks - GEN_BLOCKS
    gen_rows = GEN_BLOCKS * BLOCK
    own_refs = (up_ref, down_ref)
    side = lax.axis_index("side")
    rep = lax.axis_index("rep")
    core = rep % 2
    at_x = (rep // 2) % 2
    at_y = rep // 4
    flip = 1 - 2 * core
    rep_x = rep + 2 - 4 * at_x
    rep_y = rep + 4 - 8 * at_y
    rep_d = rep_y + 2 - 4 * at_x
    is_gen = side == 1
    is_far = side == 0
    to_z = (1 - side, rep)
    to_sib = (side, rep + flip)
    to_x = (side, rep_x)
    to_y = (side, rep_y)
    arrives = (rep, rep_x, rep_y, rep_d, rep + flip, rep_x + flip, rep_y + flip, rep_d + flip)
    my_blocks = GEN_BLOCKS * side + far_blocks * (1 - side)

    def rows(index):
        return pl.ds(pl.multiple_of(index * piece, 16), piece)

    def remote(layer, m, slot, index, target, source=None):
        there = full_ref.at[layer, m, rows(index), :]
        return pltpu.make_async_remote_copy(
            src_ref=there if source is None else source,
            dst_ref=there,
            send_sem=send.at[layer, m, slot],
            recv_sem=recv.at[layer, m, slot],
            device_id=target,
            device_id_type=MESH,
        )

    def fetch(layer, m, slot, source=None):
        where = rows(arrives[slot])
        source = full_ref.at[layer, m, where, :] if source is None else source
        return pltpu.make_async_copy(source, w_buf.at[layer % 2, m, where, :], load.at[layer % 2, m, slot])

    def arrived(layer, m, slot):
        remote(layer, m, slot, arrives[slot], to_sib).wait_recv()
        fetch(layer, m, slot).start()

    def send_z(layer):
        for m in range(2):
            remote(layer, m, Z, rep, to_z, own_refs[m].at[layer]).start()

    def spread(layer, m, source):
        remote(layer, m, X, rep, to_x, source).start()
        remote(layer, m, Y, rep, to_y, source).start()
        remote(layer, m, SIB, rep, to_sib, source).start()

    def send_own(layer, m):
        @pl.when(is_far)
        def _():
            spread(layer, m, own_refs[m].at[layer])

        @pl.when(is_gen)
        def _():
            remote(layer, m, Z, rep, to_z).wait_recv()
            spread(layer, m, None)

    def fetch_own(layer):
        for m in range(2):
            @pl.when(is_far)
            def _():
                fetch(layer, m, Z, own_refs[m].at[layer]).start()

            @pl.when(is_gen)
            def _():
                fetch(layer, m, Z).start()

    def direct(layer, m):
        arrived(layer, m, X)
        if m == 0:
            remote(layer, m, DIAG, rep_x, to_y).start()
        remote(layer, m, SIB_X, rep_x, to_sib).start()
        arrived(layer, m, Y)
        if m == 1:
            remote(layer, m, DIAG, rep_y, to_x).start()
        remote(layer, m, SIB_Y, rep_y, to_sib).start()

    def diagonal(layer, m):
        arrived(layer, m, DIAG)
        remote(layer, m, SIB_DIAG, rep_d, to_sib).start()

    def from_sibling(layer, m):
        for slot in (SIB, SIB_X, SIB_Y, SIB_DIAG):
            arrived(layer, m, slot)

    def far_x():
        return pltpu.make_async_remote_copy(
            src_ref=x_ref.at[pl.ds(gen_rows, far_blocks * BLOCK), :],
            dst_ref=h.at[pl.ds(0, far_blocks * BLOCK), :],
            send_sem=x_sem.at[0],
            recv_sem=x_sem.at[1],
            device_id=to_z,
            device_id_type=MESH,
        )

    def near_x():
        return pltpu.make_async_copy(x_ref.at[pl.ds(0, gen_rows), :], h.at[...], x_sem.at[2])

    def far_y(b):
        return pltpu.make_async_remote_copy(
            src_ref=h.at[pl.ds(pl.multiple_of(b * BLOCK, BLOCK), BLOCK), :],
            dst_ref=y_ref.at[pl.ds(pl.multiple_of(gen_rows + b * BLOCK, BLOCK), BLOCK), :],
            send_sem=y_send.at[b],
            recv_sem=y_recv.at[b],
            device_id=to_z,
            device_id_type=MESH,
        )

    def near_y(b):
        where = pl.ds(pl.multiple_of(b * BLOCK, BLOCK), BLOCK)
        return pltpu.make_async_copy(h.at[where, :], y_ref.at[where, :], y_local.at[b])

    def compute(layer, b):
        par = layer % 2
        where = pl.ds(pl.multiple_of(b * BLOCK, BLOCK), BLOCK)
        h_block = h[where, :]
        for at, size in cuts(ffn, 512):
            z = jnp.dot(h_block, w_buf[par, 0, :, at : at + size], preferred_element_type=jnp.float32)
            act[:, at : at + size] = gelu(z).astype(jnp.bfloat16)
        for at, size in cuts(width, 256):
            p = lax.dot_general(
                act[...],
                w_buf[par, 1, at : at + size, :],
                (((1,), (1,)), ((), ())),
                preferred_element_type=jnp.float32,
            )
            h[where, at : at + size] = (h[where, at : at + size].astype(jnp.float32) + p).astype(jnp.bfloat16)

    barrier = pltpu.get_barrier_semaphore()
    for target in (to_z, to_sib, to_x, to_y):
        pl.semaphore_signal(barrier, inc=1, device_id=target, device_id_type=MESH)
    pl.semaphore_wait(barrier, 4)

    @pl.when(is_far)
    def _():
        send_z(0)

    @pl.when(is_gen)
    def _():
        far_x().start()
        near_x().start()

    send_own(0, 0)
    send_own(0, 1)

    def step(s, carry):
        receiving = s < layers

        @pl.when(receiving)
        def _():
            fetch_own(s)

        @pl.when(is_far & (s + 1 < layers))
        def _():
            send_z(s + 1)

        @pl.when(is_far & (s == 1))
        def _():
            far_x().wait_recv()

        @pl.when(is_gen & (s == 1))
        def _():
            near_x().wait()

        def block(b, inner):
            @pl.when((s > 0) & (b < my_blocks))
            def _():
                compute(s - 1, b)

            @pl.when((s == layers) & (b < my_blocks) & is_gen)
            def _():
                near_y(b).start()

            @pl.when((s == layers) & (b < my_blocks) & is_far)
            def _():
                far_y(b).start()

            @pl.when(receiving & (b == 1))
            def _():
                direct(s, 0)

            @pl.when(receiving & (b == 3))
            def _():
                direct(s, 1)

            @pl.when((s + 1 < layers) & (b == 3))
            def _():
                send_own(s + 1, 0)
                send_own(s + 1, 1)

            @pl.when(receiving & (b == 4))
            def _():
                for m in range(2):
                    diagonal(s, m)
                for m in range(2):
                    from_sibling(s, m)

            return inner

        lax.fori_loop(0, GEN_BLOCKS, block, 0)

        @pl.when(receiving)
        def _():
            for m in range(2):
                for slot in range(SLOTS):
                    fetch(s, m, slot).wait()

        return carry

    lax.fori_loop(0, layers + 1, step, 0)

    @pl.when(is_gen)
    def _():
        far_x().wait_send()
        for b in range(GEN_BLOCKS):
            near_y(b).wait()
        for b in range(far_blocks):
            far_y(b).wait_recv()

    @pl.when(is_far)
    def _():
        for b in range(far_blocks):
            far_y(b).wait_send()

    def drain(layer, carry):
        for m in range(2):
            @pl.when(is_far)
            def _():
                remote(layer, m, Z, rep, to_z).wait_send()

            for slot in range(1, SLOTS):
                remote(layer, m, slot, rep, to_sib).wait_send()
        return carry

    lax.fori_loop(0, layers, drain, 0)


def mlp_stack(up, down, x):
    layers, piece, ffn = up.shape
    tokens, width = x.shape
    hbm = pl.BlockSpec(memory_space=pltpu.HBM)
    dma = pltpu.SemaphoreType.DMA
    _, y = pl.pallas_call(
        stack_kernel,
        in_specs=[hbm] * 3,
        out_specs=[hbm] * 2,
        out_shape=[
            jax.ShapeDtypeStruct((layers, 2, width, ffn), jnp.bfloat16),
            jax.ShapeDtypeStruct((tokens, width), jnp.bfloat16),
        ],
        scratch_shapes=[
            pltpu.VMEM((2, 2, width, ffn), jnp.bfloat16),
            pltpu.VMEM((BLOCK, ffn), jnp.bfloat16),
            pltpu.VMEM((GEN_BLOCKS * BLOCK, width), jnp.bfloat16),
            dma((layers, 2, SLOTS)),
            dma((layers, 2, SLOTS)),
            dma((2, 2, SLOTS)),
            dma((3,)),
            dma((GEN_BLOCKS,)),
            dma((GEN_BLOCKS,)),
            dma((GEN_BLOCKS,)),
        ],
        compiler_params=pltpu.CompilerParams(
            collective_id=0, has_side_effects=True, vmem_limit_bytes=60 * 2**20
        ),
        name="mlp_stack",
    )(up, down, x)
    return y


def solution(mesh):
    up_spec = P("side", None, "rep", None)
    down_spec = P("side", None, None, "rep")
    act_spec = P("side", "rep", None)

    def device_step(w_up, w_down, g_up, g_down, learn_rate, prompts, prompt_lens):
        is_gen = lax.axis_index("side") == 1
        tokens = prompts.shape[1]
        new_up = w_up - learn_rate * g_up
        new_down = w_down - learn_rate * g_down
        up_bf = new_up[0].astype(jnp.bfloat16)
        down_bf = jnp.swapaxes(new_down[0], 1, 2).astype(jnp.bfloat16)
        out = mlp_stack(up_bf, down_bf, prompts[0])
        keep = (jnp.arange(tokens)[:, None] < prompt_lens[0]) & is_gen
        out = jnp.where(keep, out, jnp.zeros_like(out))
        return new_up, new_down, out[None]

    return jax.shard_map(
        device_step,
        mesh=mesh,
        in_specs=(up_spec, down_spec, up_spec, down_spec, P(), act_spec, P("rep")),
        out_specs=(up_spec, down_spec, act_spec),
        check_vma=False,
    )
```

```python
import functools

import jax
import jax.numpy as jnp
from jax import lax
from jax.experimental import pallas as pl
from jax.experimental.pallas import tpu as pltpu
from jax.sharding import PartitionSpec as P

ROOT_2_PI = 0.7978845608
CUBIC = 0.044715 * ROOT_2_PI
MESH = pl.DeviceIdType.MESH
BLOCK = 256
GEN_BLOCKS = 10
HANDED = 2
DIRECT_AT = (0, 2)
OWN_AT = (0, 2)
DIAG_AT = 8
SIB_AT = 9
Z_AHEAD = 2
PARTS = 2
Z, X, Y, DIAG, SIB, SIB_X, SIB_Y, SIB_DIAG = range(8)
SLOTS = 8


def gelu(z):
    half = 0.5 * z
    return half + half * jnp.tanh(z * (ROOT_2_PI + CUBIC * (z * z)))


def cuts(total, step):
    return [(at, min(step, total - at)) for at in range(0, total, step)]


def stack_kernel(
    up_ref, down_ref, first_ref, x_ref, full_ref, y_ref, w_buf, act, acc, h, send, recv, load, x_sem, hand_send, hand_recv, y_send, y_recv, y_local
):
    steps, _, width, ffn = full_ref.shape
    piece = up_ref.shape[1]
    tokens = x_ref.shape[0]
    blocks = tokens // BLOCK
    far_blocks = blocks - GEN_BLOCKS
    gen_rows = GEN_BLOCKS * BLOCK
    own_refs = (up_ref, down_ref)
    side = lax.axis_index("side")
    rep = lax.axis_index("rep")
    core = rep % 2
    at_x = (rep // 2) % 2
    at_y = rep // 4
    flip = 1 - 2 * core
    rep_x = rep + 2 - 4 * at_x
    rep_y = rep + 4 - 8 * at_y
    rep_d = rep_y + 2 - 4 * at_x
    is_gen = side == 1
    is_far = side == 0
    to_z = (1 - side, rep)
    to_sib = (side, rep + flip)
    to_x = (side, rep_x)
    to_y = (side, rep_y)
    arrives = (rep, rep_x, rep_y, rep_d, rep + flip, rep_x + flip, rep_y + flip, rep_d + flip)
    my_blocks = GEN_BLOCKS * side + far_blocks * (1 - side)
    all_blocks = GEN_BLOCKS + HANDED

    def rows(index):
        return pl.ds(pl.multiple_of(index * piece, 16), piece)

    def remote(turn, m, slot, index, target, source=None):
        there = full_ref.at[turn, m, rows(index), :]
        return pltpu.make_async_remote_copy(
            src_ref=there if source is None else source,
            dst_ref=there,
            send_sem=send.at[turn, m, slot],
            recv_sem=recv.at[turn, m, slot],
            device_id=target,
            device_id_type=MESH,
        )

    def own(turn, m):
        columns = pl.ds(pl.multiple_of(turn % PARTS * ffn, 128), ffn)
        return own_refs[m].at[turn // PARTS, :, columns]

    def fetch(turn, m, slot, source=None):
        where = rows(arrives[slot])
        source = full_ref.at[turn, m, where, :] if source is None else source
        return pltpu.make_async_copy(source, w_buf.at[turn % 2, m, where, :], load.at[turn % 2, m, slot])

    def received(turn, m, slot):
        remote(turn, m, slot, arrives[slot], to_sib).wait_recv()

    def arrived(turn, m, slot):
        received(turn, m, slot)
        fetch(turn, m, slot).start()

    def send_z(turn):
        for m in range(2):
            remote(turn, m, Z, rep, to_z, own(turn, m)).start()

    def spread(turn, m, source):
        remote(turn, m, X, rep, to_x, source).start()
        remote(turn, m, Y, rep, to_y, source).start()
        remote(turn, m, SIB, rep, to_sib, source).start()

    def send_own(turn, m, first=False):
        @pl.when(is_far)
        def _():
            spread(turn, m, own(turn, m))

        @pl.when(is_gen)
        def _():
            if first:
                spread(turn, m, first_ref.at[m])
            else:
                received(turn, m, Z)
                spread(turn, m, None)

    def fetch_own(turn):
        for m in range(2):
            @pl.when(is_far)
            def _():
                fetch(turn, m, Z, own(turn, m)).start()

            @pl.when(is_gen & (turn == 0))
            def _():
                fetch(turn, m, Z, first_ref.at[m]).start()

            @pl.when(is_gen & (turn > 0))
            def _():
                fetch(turn, m, Z).start()

    def direct(turn, m):
        received(turn, m, X)
        if m == 0:
            remote(turn, m, DIAG, rep_x, to_y).start()
        remote(turn, m, SIB_X, rep_x, to_sib).start()
        received(turn, m, Y)
        if m == 1:
            remote(turn, m, DIAG, rep_y, to_x).start()
        remote(turn, m, SIB_Y, rep_y, to_sib).start()

    def diagonal(turn, m):
        fetch(turn, m, X).start()
        fetch(turn, m, Y).start()
        arrived(turn, m, DIAG)
        remote(turn, m, SIB_DIAG, rep_d, to_sib).start()

    def from_sibling(turn, m):
        for slot in (SIB, SIB_X, SIB_Y, SIB_DIAG):
            arrived(turn, m, slot)

    def far_x():
        return pltpu.make_async_remote_copy(
            src_ref=x_ref.at[pl.ds(gen_rows, far_blocks * BLOCK), :],
            dst_ref=h.at[pl.ds(0, far_blocks * BLOCK), :],
            send_sem=x_sem.at[0],
            recv_sem=x_sem.at[1],
            device_id=to_z,
            device_id_type=MESH,
        )

    def near_x():
        return pltpu.make_async_copy(x_ref.at[pl.ds(0, gen_rows), :], h.at[pl.ds(0, gen_rows), :], x_sem.at[2])

    def hand(b):
        return pltpu.make_async_remote_copy(
            src_ref=h.at[pl.ds(pl.multiple_of(b * BLOCK, BLOCK), BLOCK), :],
            dst_ref=h.at[pl.ds(pl.multiple_of(gen_rows + b * BLOCK, BLOCK), BLOCK), :],
            send_sem=hand_send.at[b],
            recv_sem=hand_recv.at[b],
            device_id=to_z,
            device_id_type=MESH,
        )

    def far_y(b):
        return pltpu.make_async_remote_copy(
            src_ref=h.at[pl.ds(pl.multiple_of(b * BLOCK, BLOCK), BLOCK), :],
            dst_ref=y_ref.at[pl.ds(pl.multiple_of(gen_rows + b * BLOCK, BLOCK), BLOCK), :],
            send_sem=y_send.at[b],
            recv_sem=y_recv.at[b],
            device_id=to_z,
            device_id_type=MESH,
        )

    def near_y(b):
        where = pl.ds(pl.multiple_of(b * BLOCK, BLOCK), BLOCK)
        return pltpu.make_async_copy(h.at[where, :], y_ref.at[where, :], y_local.at[b])

    def compute(turn, b, part):
        par = turn % 2
        where = pl.ds(pl.multiple_of(b * BLOCK, BLOCK), BLOCK)
        h_block = h[where, :]
        for at, size in cuts(ffn, 512):
            z = jnp.dot(h_block, w_buf[par, 0, :, at : at + size], preferred_element_type=jnp.float32)
            act[:, at : at + size] = gelu(z).astype(jnp.bfloat16)
        for at, size in cuts(width, 256):
            p = lax.dot_general(
                act[...],
                w_buf[par, 1, at : at + size, :],
                (((1,), (1,)), ((), ())),
                preferred_element_type=jnp.float32,
            )
            if part < PARTS - 1:
                acc[where, at : at + size] = p if part == 0 else acc[where, at : at + size] + p
            else:
                p = acc[where, at : at + size] + p
                h[where, at : at + size] = (h[where, at : at + size].astype(jnp.float32) + p).astype(jnp.bfloat16)

    barrier = pltpu.get_barrier_semaphore()
    for target in (to_z, to_sib, to_x, to_y):
        pl.semaphore_signal(barrier, inc=1, device_id=target, device_id_type=MESH)
    pl.semaphore_wait(barrier, 4)

    @pl.when(is_far)
    def _():
        for ahead in range(1, Z_AHEAD):
            send_z(ahead)

    @pl.when(is_gen)
    def _():
        far_x().start()
        near_x().start()

    send_own(0, 0, True)
    send_own(0, 1, True)

    def step(s, carry):
        ready = s
        done = s - 1
        receiving = s < steps
        closing = receiving
        last = done == steps - 1
        tail = jnp.where(done >= steps - PARTS, HANDED, 0)
        low = tail * (1 - side)
        high = my_blocks + tail * side

        @pl.when(closing)
        def _():
            fetch_own(ready)

        @pl.when(is_far & (s + Z_AHEAD < steps))
        def _():
            send_z(s + Z_AHEAD)

        @pl.when(is_far & (done == 0))
        def _():
            far_x().wait_recv()

        @pl.when(is_gen & (done == 0))
        def _():
            near_x().wait()

        def block(b, inner):
            for m in range(2):
                @pl.when(receiving & (b == DIRECT_AT[m]))
                def _():
                    direct(s, m)

                @pl.when((s + 1 < steps) & (b == OWN_AT[m]))
                def _():
                    send_own(s + 1, m)

            @pl.when(closing & (b == DIAG_AT))
            def _():
                for m in range(2):
                    diagonal(ready, m)

            @pl.when(closing & (b == SIB_AT))
            def _():
                for m in range(2):
                    from_sibling(ready, m)

            mine = (b >= low) & (b < high)

            @pl.when(is_gen & (done == steps - PARTS) & mine & (b >= GEN_BLOCKS))
            def _():
                hand(b - GEN_BLOCKS).wait_recv()

            for part in range(PARTS):
                @pl.when((done >= 0) & (done % PARTS == part) & mine)
                def _():
                    compute(done, b, part)

            @pl.when(is_far & (done == steps - PARTS - 1) & (b < HANDED))
            def _():
                hand(b).start()

            @pl.when(last & mine & is_gen)
            def _():
                near_y(b).start()

            @pl.when(last & mine & is_far)
            def _():
                far_y(b).start()

            return inner

        lax.fori_loop(0, all_blocks, block, 0)

        @pl.when(closing)
        def _():
            for m in range(2):
                for slot in range(SLOTS):
                    fetch(ready, m, slot).wait()

        return carry

    lax.fori_loop(0, steps + 1, step, 0)

    @pl.when(is_gen)
    def _():
        far_x().wait_send()
        for b in range(all_blocks):
            near_y(b).wait()
        for b in range(HANDED, far_blocks):
            far_y(b).wait_recv()

    @pl.when(is_far)
    def _():
        for b in range(HANDED):
            hand(b).wait_send()
        for b in range(HANDED, far_blocks):
            far_y(b).wait_send()

    def drain(turn, carry):
        for m in range(2):
            @pl.when(is_far & (turn > 0))
            def _():
                remote(turn, m, Z, rep, to_z).wait_send()

            for slot in range(1, SLOTS):
                remote(turn, m, slot, rep, to_sib).wait_send()
        return carry

    lax.fori_loop(0, steps, drain, 0)


def mlp_stack(up, down, first, x):
    layers, piece, ffn = up.shape
    tokens, width = x.shape
    steps, ffn = layers * PARTS, ffn // PARTS
    hbm = pl.BlockSpec(memory_space=pltpu.HBM)
    dma = pltpu.SemaphoreType.DMA
    _, y = pl.pallas_call(
        stack_kernel,
        in_specs=[hbm] * 4,
        out_specs=[hbm] * 2,
        out_shape=[
            jax.ShapeDtypeStruct((steps, 2, width, ffn), jnp.bfloat16),
            jax.ShapeDtypeStruct((tokens, width), jnp.bfloat16),
        ],
        scratch_shapes=[
            pltpu.VMEM((2, 2, width, ffn), jnp.bfloat16),
            pltpu.VMEM((BLOCK, ffn), jnp.bfloat16),
            pltpu.VMEM(((GEN_BLOCKS + HANDED) * BLOCK, width), jnp.float32),
            pltpu.VMEM(((GEN_BLOCKS + HANDED) * BLOCK, width), jnp.bfloat16),
            dma((steps, 2, SLOTS)),
            dma((steps, 2, SLOTS)),
            dma((2, 2, SLOTS)),
            dma((3,)),
            dma((HANDED,)),
            dma((HANDED,)),
            dma((tokens // BLOCK,)),
            dma((tokens // BLOCK,)),
            dma((tokens // BLOCK,)),
        ],
        compiler_params=pltpu.CompilerParams(
            collective_id=0, has_side_effects=True, vmem_limit_bytes=60 * 2**20
        ),
        name="mlp_stack",
    )(up, down, first, x)
    return y


def solution(mesh):
    up_spec = P("side", None, "rep", None)
    down_spec = P("side", None, None, "rep")
    act_spec = P("side", "rep", None)

    def device_step(w_up, w_down, g_up, g_down, learn_rate, prompts, prompt_lens):
        is_gen = lax.axis_index("side") == 1
        tokens = prompts.shape[1]
        part = w_up.shape[3] // PARTS
        first_up = w_up[0, 0, :, :part] - learn_rate * g_up[0, 0, :, :part]
        first_down = (w_down[0, 0, :part] - learn_rate * g_down[0, 0, :part]).T
        first = jnp.stack([first_up.astype(jnp.bfloat16), first_down.astype(jnp.bfloat16)])
        first, w_up, w_down = lax.optimization_barrier((first, w_up, w_down))
        first = lax.ppermute(first, "side", [(0, 1)])
        new_up = w_up - learn_rate * g_up
        new_down = w_down - learn_rate * g_down
        up_bf = new_up[0].astype(jnp.bfloat16)
        down_bf = jnp.swapaxes(new_down[0], 1, 2).astype(jnp.bfloat16)
        out = mlp_stack(up_bf, down_bf, first, prompts[0])
        keep = (jnp.arange(tokens)[:, None] < prompt_lens[0]) & is_gen
        out = jnp.where(keep, out, jnp.zeros_like(out))
        return new_up, new_down, out[None]

    return jax.shard_map(
        device_step,
        mesh=mesh,
        in_specs=(up_spec, down_spec, up_spec, down_spec, P(), act_spec, P("rep")),
        out_specs=(up_spec, down_spec, act_spec),
        check_vma=False,
    )
```

```python
import functools

import jax
import jax.numpy as jnp
from jax import lax
from jax.experimental import pallas as pl
from jax.experimental.pallas import tpu as pltpu
from jax.sharding import PartitionSpec as P

ROOT_2_PI = 0.7978845608
CUBIC = 0.044715 * ROOT_2_PI
MESH = pl.DeviceIdType.MESH
BLOCK = 256
GEN_BLOCKS = 10
HANDED = 2
DIRECT_AT = (1, 3)
OWN_AT = (1, 3)
DIAG_AT = 9
SIB_AT = 9
Z_AHEAD = 2
PARTS = 2
Z, X, Y, DIAG, SIB, SIB_X, SIB_Y, SIB_DIAG = range(8)
SLOTS = 8


def gelu(z):
    half = 0.5 * z
    return half + half * jnp.tanh(z * (ROOT_2_PI + CUBIC * (z * z)))


def cuts(total, step):
    return [(at, min(step, total - at)) for at in range(0, total, step)]


def stack_kernel(
    up_ref, down_ref, first_ref, x_ref, full_ref, y_ref, w_buf, act, acc, h, send, recv, load, x_sem, hand_send, hand_recv, y_send, y_recv, y_local
):
    steps, _, width, ffn = full_ref.shape
    piece = up_ref.shape[1]
    tokens = x_ref.shape[0]
    blocks = tokens // BLOCK
    far_blocks = blocks - GEN_BLOCKS
    gen_rows = GEN_BLOCKS * BLOCK
    own_refs = (up_ref, down_ref)
    side = lax.axis_index("side")
    rep = lax.axis_index("rep")
    core = rep % 2
    at_x = (rep // 2) % 2
    at_y = rep // 4
    flip = 1 - 2 * core
    rep_x = rep + 2 - 4 * at_x
    rep_y = rep + 4 - 8 * at_y
    rep_d = rep_y + 2 - 4 * at_x
    is_gen = side == 1
    is_far = side == 0
    to_z = (1 - side, rep)
    to_sib = (side, rep + flip)
    to_x = (side, rep_x)
    to_y = (side, rep_y)
    arrives = (rep, rep_x, rep_y, rep_d, rep + flip, rep_x + flip, rep_y + flip, rep_d + flip)
    my_blocks = GEN_BLOCKS * side + far_blocks * (1 - side)
    all_blocks = GEN_BLOCKS + HANDED

    def rows(index):
        return pl.ds(pl.multiple_of(index * piece, 16), piece)

    def remote(turn, m, slot, index, target, source=None):
        there = full_ref.at[turn, m, rows(index), :]
        return pltpu.make_async_remote_copy(
            src_ref=there if source is None else source,
            dst_ref=there,
            send_sem=send.at[turn, m, slot],
            recv_sem=recv.at[turn, m, slot],
            device_id=target,
            device_id_type=MESH,
        )

    def own(turn, m):
        columns = pl.ds(pl.multiple_of(turn % PARTS * ffn, 128), ffn)
        return own_refs[m].at[turn // PARTS, :, columns]

    def fetch(turn, m, slot, source=None):
        where = rows(arrives[slot])
        source = full_ref.at[turn, m, where, :] if source is None else source
        return pltpu.make_async_copy(source, w_buf.at[turn % 2, m, where, :], load.at[turn % 2, m, slot])

    def received(turn, m, slot):
        remote(turn, m, slot, arrives[slot], to_sib).wait_recv()

    def arrived(turn, m, slot):
        received(turn, m, slot)
        fetch(turn, m, slot).start()

    def send_z(turn):
        for m in range(2):
            remote(turn, m, Z, rep, to_z, own(turn, m)).start()

    def spread(turn, m, source):
        remote(turn, m, X, rep, to_x, source).start()
        remote(turn, m, Y, rep, to_y, source).start()
        remote(turn, m, SIB, rep, to_sib, source).start()

    def send_own(turn, m, first=False):
        @pl.when(is_far)
        def _():
            spread(turn, m, own(turn, m))

        @pl.when(is_gen)
        def _():
            if first:
                spread(turn, m, first_ref.at[m])
            else:
                received(turn, m, Z)
                spread(turn, m, None)

    def fetch_own(turn):
        for m in range(2):
            @pl.when(is_far)
            def _():
                fetch(turn, m, Z, own(turn, m)).start()

            @pl.when(is_gen & (turn == 0))
            def _():
                fetch(turn, m, Z, first_ref.at[m]).start()

            @pl.when(is_gen & (turn > 0))
            def _():
                fetch(turn, m, Z).start()

    def direct(turn, m):
        received(turn, m, X)
        if m == 0:
            remote(turn, m, DIAG, rep_x, to_y).start()
        remote(turn, m, SIB_X, rep_x, to_sib).start()
        received(turn, m, Y)
        if m == 1:
            remote(turn, m, DIAG, rep_y, to_x).start()
        remote(turn, m, SIB_Y, rep_y, to_sib).start()

    def diagonal(turn, m):
        fetch(turn, m, X).start()
        fetch(turn, m, Y).start()
        arrived(turn, m, DIAG)
        remote(turn, m, SIB_DIAG, rep_d, to_sib).start()

    def from_sibling(turn, m):
        for slot in (SIB, SIB_X, SIB_Y, SIB_DIAG):
            arrived(turn, m, slot)

    def far_x():
        return pltpu.make_async_remote_copy(
            src_ref=x_ref.at[pl.ds(gen_rows, far_blocks * BLOCK), :],
            dst_ref=h.at[pl.ds(0, far_blocks * BLOCK), :],
            send_sem=x_sem.at[0],
            recv_sem=x_sem.at[1],
            device_id=to_z,
            device_id_type=MESH,
        )

    def near_x():
        return pltpu.make_async_copy(x_ref.at[pl.ds(0, gen_rows), :], h.at[pl.ds(0, gen_rows), :], x_sem.at[2])

    def hand(b):
        return pltpu.make_async_remote_copy(
            src_ref=h.at[pl.ds(pl.multiple_of(b * BLOCK, BLOCK), BLOCK), :],
            dst_ref=h.at[pl.ds(pl.multiple_of(gen_rows + b * BLOCK, BLOCK), BLOCK), :],
            send_sem=hand_send.at[b],
            recv_sem=hand_recv.at[b],
            device_id=to_z,
            device_id_type=MESH,
        )

    def far_y(b):
        return pltpu.make_async_remote_copy(
            src_ref=h.at[pl.ds(pl.multiple_of(b * BLOCK, BLOCK), BLOCK), :],
            dst_ref=y_ref.at[pl.ds(pl.multiple_of(gen_rows + b * BLOCK, BLOCK), BLOCK), :],
            send_sem=y_send.at[b],
            recv_sem=y_recv.at[b],
            device_id=to_z,
            device_id_type=MESH,
        )

    def near_y(b):
        where = pl.ds(pl.multiple_of(b * BLOCK, BLOCK), BLOCK)
        return pltpu.make_async_copy(h.at[where, :], y_ref.at[where, :], y_local.at[b])

    def compute(turn, b, part):
        par = turn % 2
        where = pl.ds(pl.multiple_of(b * BLOCK, BLOCK), BLOCK)
        h_block = h[where, :]
        for at, size in cuts(ffn, 512):
            z = jnp.dot(h_block, w_buf[par, 0, :, at : at + size], preferred_element_type=jnp.float32)
            act[:, at : at + size] = gelu(z).astype(jnp.bfloat16)
        for at, size in cuts(width, 256):
            p = lax.dot_general(
                act[...],
                w_buf[par, 1, at : at + size, :],
                (((1,), (1,)), ((), ())),
                preferred_element_type=jnp.float32,
            )
            if part < PARTS - 1:
                acc[where, at : at + size] = p if part == 0 else acc[where, at : at + size] + p
            else:
                p = acc[where, at : at + size] + p
                h[where, at : at + size] = (h[where, at : at + size].astype(jnp.float32) + p).astype(jnp.bfloat16)

    barrier = pltpu.get_barrier_semaphore()
    for target in (to_z, to_sib, to_x, to_y):
        pl.semaphore_signal(barrier, inc=1, device_id=target, device_id_type=MESH)
    pl.semaphore_wait(barrier, 4)

    @pl.when(is_far)
    def _():
        for ahead in range(1, Z_AHEAD):
            send_z(ahead)

    @pl.when(is_gen)
    def _():
        far_x().start()
        near_x().start()

    send_own(0, 0, True)
    send_own(0, 1, True)

    def step(s, carry):
        ready = s
        done = s - 1
        receiving = s < steps
        closing = receiving
        last = done == steps - 1
        tail = jnp.where(done >= steps - PARTS, HANDED, 0)
        low = tail * (1 - side)
        high = my_blocks + tail * side

        @pl.when(closing)
        def _():
            fetch_own(ready)

        @pl.when(is_far & (s + Z_AHEAD < steps))
        def _():
            send_z(s + Z_AHEAD)

        @pl.when(is_far & (done == 0))
        def _():
            far_x().wait_recv()

        @pl.when(is_gen & (done == 0))
        def _():
            near_x().wait()

        def block(b, inner):
            for m in range(2):
                @pl.when(receiving & (b == DIRECT_AT[m]))
                def _():
                    direct(s, m)

                @pl.when((s + 1 < steps) & (b == OWN_AT[m]))
                def _():
                    send_own(s + 1, m)

            @pl.when(closing & (b == DIAG_AT))
            def _():
                for m in range(2):
                    diagonal(ready, m)

            @pl.when(closing & (b == SIB_AT))
            def _():
                for m in range(2):
                    from_sibling(ready, m)

            mine = (b >= low) & (b < high)

            @pl.when(is_gen & (done == steps - PARTS) & mine & (b >= GEN_BLOCKS))
            def _():
                hand(b - GEN_BLOCKS).wait_recv()

            for part in range(PARTS):
                @pl.when((done >= 0) & (done % PARTS == part) & mine)
                def _():
                    compute(done, b, part)

            @pl.when(is_far & (done == steps - PARTS - 1) & (b < HANDED))
            def _():
                hand(b).start()

            @pl.when(last & mine & is_gen)
            def _():
                near_y(b).start()

            @pl.when(last & mine & is_far)
            def _():
                far_y(b).start()

            return inner

        lax.fori_loop(0, all_blocks, block, 0)

        @pl.when(closing)
        def _():
            for m in range(2):
                for slot in range(SLOTS):
                    fetch(ready, m, slot).wait()

        return carry

    lax.fori_loop(0, steps + 1, step, 0)

    @pl.when(is_gen)
    def _():
        far_x().wait_send()
        for b in range(all_blocks):
            near_y(b).wait()
        for b in range(HANDED, far_blocks):
            far_y(b).wait_recv()

    @pl.when(is_far)
    def _():
        for b in range(HANDED):
            hand(b).wait_send()
        for b in range(HANDED, far_blocks):
            far_y(b).wait_send()

    def drain(turn, carry):
        for m in range(2):
            @pl.when(is_far & (turn > 0))
            def _():
                remote(turn, m, Z, rep, to_z).wait_send()

            for slot in range(1, SLOTS):
                remote(turn, m, slot, rep, to_sib).wait_send()
        return carry

    lax.fori_loop(0, steps, drain, 0)


def update_kernel(rate_ref, w_up, g_up, w_down, g_down, new_up, new_down, up_bf, down_bf):
    rate = rate_ref[0]
    for w, g, new, rounded in ((w_up, g_up, new_up, up_bf), (w_down, g_down, new_down, down_bf)):
        value = w[...] - rate * g[...]
        new[...] = value
        rounded[...] = value.astype(jnp.bfloat16)


def update(rate, *arrays):
    layers, piece, ffn = arrays[0].shape
    block = pl.BlockSpec((1, piece, ffn // PARTS), lambda layer, part: (layer, 0, part))
    kinds = (jnp.float32, jnp.float32, jnp.bfloat16, jnp.bfloat16)
    return pl.pallas_call(
        update_kernel,
        grid=(layers, PARTS),
        in_specs=[pl.BlockSpec(memory_space=pltpu.SMEM)] + [block] * 4,
        out_specs=[block] * 4,
        out_shape=[jax.ShapeDtypeStruct((layers, piece, ffn), kind) for kind in kinds],
        compiler_params=pltpu.CompilerParams(vmem_limit_bytes=62 * 2**20),
        cost_estimate=pl.CostEstimate(
            flops=60 * layers * piece * ffn, bytes_accessed=28 * layers * piece * ffn, transcendentals=0
        ),
        name="update",
    )(rate.reshape(1), *arrays)


def mlp_stack(up, down, first, x):
    layers, piece, ffn = up.shape
    tokens, width = x.shape
    steps, ffn = layers * PARTS, ffn // PARTS
    hbm = pl.BlockSpec(memory_space=pltpu.HBM)
    dma = pltpu.SemaphoreType.DMA
    _, y = pl.pallas_call(
        stack_kernel,
        in_specs=[hbm] * 4,
        out_specs=[hbm] * 2,
        out_shape=[
            jax.ShapeDtypeStruct((steps, 2, width, ffn), jnp.bfloat16),
            jax.ShapeDtypeStruct((tokens, width), jnp.bfloat16),
        ],
        scratch_shapes=[
            pltpu.VMEM((2, 2, width, ffn), jnp.bfloat16),
            pltpu.VMEM((BLOCK, ffn), jnp.bfloat16),
            pltpu.VMEM(((GEN_BLOCKS + HANDED) * BLOCK, width), jnp.float32),
            pltpu.VMEM(((GEN_BLOCKS + HANDED) * BLOCK, width), jnp.bfloat16),
            dma((steps, 2, SLOTS)),
            dma((steps, 2, SLOTS)),
            dma((2, 2, SLOTS)),
            dma((3,)),
            dma((HANDED,)),
            dma((HANDED,)),
            dma((tokens // BLOCK,)),
            dma((tokens // BLOCK,)),
            dma((tokens // BLOCK,)),
        ],
        compiler_params=pltpu.CompilerParams(
            collective_id=0, has_side_effects=True, vmem_limit_bytes=60 * 2**20
        ),
        name="mlp_stack",
    )(up, down, first, x)
    return y


def solution(mesh):
    up_spec = P("side", None, "rep", None)
    down_spec = P("side", None, None, "rep")
    act_spec = P("side", "rep", None)

    def device_step(w_up, w_down, g_up, g_down, learn_rate, prompts, prompt_lens):
        is_gen = lax.axis_index("side") == 1
        tokens = prompts.shape[1]
        part = w_up.shape[3] // PARTS
        first_up = w_up[0, 0, :, :part] - learn_rate * g_up[0, 0, :, :part]
        first_down = (w_down[0, 0, :part] - learn_rate * g_down[0, 0, :part]).T
        first = jnp.stack([first_up.astype(jnp.bfloat16), first_down.astype(jnp.bfloat16)])
        first, w_up, w_down = lax.optimization_barrier((first, w_up, w_down))
        first = lax.ppermute(first, "side", [(0, 1)])
        new_up, new_down, up_bf, down_bf = update(
            learn_rate, w_up[0], g_up[0], jnp.swapaxes(w_down[0], 1, 2), jnp.swapaxes(g_down[0], 1, 2)
        )
        out = mlp_stack(up_bf, down_bf, first, prompts[0])
        keep = (jnp.arange(tokens)[:, None] < prompt_lens[0]) & is_gen
        out = jnp.where(keep, out, jnp.zeros_like(out))
        return new_up[None], jnp.swapaxes(new_down, 1, 2)[None], out[None]

    return jax.shard_map(
        device_step,
        mesh=mesh,
        in_specs=(up_spec, down_spec, up_spec, down_spec, P(), act_spec, P("rep")),
        out_specs=(up_spec, down_spec, act_spec),
        check_vma=False,
    )
```
